512 devices in a mesh: dp: 64 (over y, z), tensor: 8 (over x, core).
Axes of the slice: x: 4, y: 4, z: 16, core: 2. Of those that a mesh axis runs over, the one named last changes fastest.
Arguments:
- inputs: bfloat16 [36864, 8192], P('dp', 'tensor'), may hold values from -6 to 6
- out_grads: bfloat16 [36864, 11264], P('dp', 'tensor'), may hold values from -600 to 600
- basis: bfloat16 [8192, 512], P('dp', 'tensor'), may hold values from -40 to 40
- weight: bfloat16 [8192, 11264], P('dp', 'tensor'), may hold values from -0.099609375 to 0.099609375
- first_moment: float32 [512, 11264], P('dp', 'tensor'), may hold values from -0.9 to 0.9
- second_moment: float32 [512, 11264], P('dp', 'tensor'), may hold values from 0.01 to 1
Outputs:
- new_weight: bfloat16 [8192, 11264], P('dp', 'tensor')
- new_first: float32 [512, 11264], P('dp', 'tensor')
- new_second: float32 [512, 11264], P('dp', 'tensor')
The draws below stay inside these ranges and needn't reach their ends.
All inputs are finite; a program needn't handle non-finite values.
Results may differ from the reference program's by a relative error of at most 0.0087.
Values may be sent and summed in bfloat16 or wider, within the bound.
No kernel may reach another device: no remote copies, remote signals or barrier semaphores. Data moves between devices by JAX's collectives and lax.ppermute only.
A program may use at most 64 MiB of HBM per device.

```python
import math
import jax
import jax.numpy as jnp
from jax import lax

D = 8192
FW = 11264
R = 512
TOKENS = 36864


def rising(key, count):
    place = jnp.arange(count, dtype=jnp.float32) / count
    jitter = jnp.exp(jax.random.uniform(key, (count,), jnp.float32, -0.6931, 0.6931))
    return 10.0 ** place * jitter


def draw_basis(key, part):
    first_key, second_key = jax.random.split(jax.random.fold_in(key, 17))
    entries = jnp.clip(jax.random.normal(first_key, (D, R), jnp.float32), -2.0, 2.0)
    scales = rising(second_key, R)
    return (entries * scales[None, :]).astype(jnp.bfloat16)


def draw_out_grads(key, part):
    keys = jax.random.split(jax.random.fold_in(key, 29), 3)
    token_scales = jnp.exp(jax.random.uniform(keys[0], (TOKENS,), jnp.float32, 0.0, 2.3026))
    column_scales = rising(keys[1], FW)
    entries = jnp.clip(jax.random.normal(keys[2], (TOKENS, FW), jnp.float32), -3.0, 3.0)
    return (entries * token_scales[:, None] * column_scales[None, :]).astype(jnp.bfloat16)


def steps_of(rng, extent, cuts, least, high):
    def one(axis_at, parts):
        steps = jax.random.uniform(jax.random.fold_in(jax.random.fold_in(rng, 6), axis_at), (parts,), jnp.float32, least / len(cuts), high / len(cuts))
        return jnp.repeat(jnp.exp(steps), extent[axis_at] // parts).reshape((-1,) + (1,) * (len(extent) - axis_at - 1))

    factor_of = one(*cuts[0])
    for cut in cuts[1:]:
        factor_of = factor_of * one(*cut)
    return factor_of


def noise(stream_key, shape, spread, bound, cuts=(), kind=jnp.bfloat16):
    drawn = spread * jax.random.normal(stream_key, shape, jnp.float32)
    if cuts:
        drawn = drawn * steps_of(stream_key, shape, cuts, -0.22, 0.18)
    return jnp.clip(drawn, -bound, bound).astype(kind)


def setup_inputs(seed: int = 0) -> dict:
    key_of = jax.random.split(jax.random.key(seed), 7)
    inputs = noise(key_of[0], (TOKENS, D), 1.0, 6.0, ((0, 64), (1, 8)))
    out_grads = draw_out_grads(jax.random.fold_in(key_of[6], 71), 0)
    basis = draw_basis(jax.random.fold_in(key_of[6], 71), 0)
    weight = noise(key_of[3], (D, FW), 0.02, 0.099609375, ((0, 64), (1, 8)))
    first_moment = noise(key_of[4], (R, FW), 0.15, 0.9, ((0, 64), (1, 8)), jnp.float32)
    second_moment = jnp.clip(jnp.exp(math.log(1.0) - 4.6051702 * jax.random.uniform(key_of[5], (R, FW), jnp.float32) ** steps_of(key_of[5], (R, FW), ((0, 64), (1, 8)), -0.2, 0.2)), 0.01, 1.0)
    return {"inputs": inputs, "out_grads": out_grads, "basis": basis, "weight": weight, "first_moment": first_moment, "second_moment": second_moment}


beta_one = 0.9
beta_two = 0.999
adam_eps = 1e-08
corr_one = 1.0 - 0.9 ** 10
corr_two = 1.0 - 0.999 ** 10
step_size = 0.002
decay_keep = 0.99

def adam_update(lowrank, square, first_moment, second_moment):
    bound_norm = math.sqrt(R * FW)
    factor = jnp.minimum(1.0, bound_norm / (jnp.sqrt(square) + 1e-06))
    clipped = lowrank * factor
    first = beta_one * first_moment + (1.0 - beta_one) * clipped
    second = beta_two * second_moment + (1.0 - beta_two) * clipped * clipped
    update = (first / corr_one / (jnp.sqrt(second / corr_two) + adam_eps)).astype(jnp.bfloat16)
    return (first, second, update)

def reference(inputs, out_grads, basis, weight, first_moment, second_moment):
    projected = jnp.dot(inputs, basis, preferred_element_type=jnp.float32).astype(jnp.bfloat16)
    lowrank = lax.dot_general(projected, out_grads, (((0,), (0,)), ((), ())), preferred_element_type=jnp.float32)
    square = jnp.sum(lowrank * lowrank)
    first, second, update = adam_update(lowrank, square, first_moment, second_moment)
    delta = jnp.dot(basis, update, preferred_element_type=jnp.float32)
    new_weight = (decay_keep * weight.astype(jnp.float32) - step_size * delta).astype(jnp.bfloat16)
    return (new_weight, first, second)
```

```python
import math

import jax
import jax.numpy as jnp
from jax import lax
from jax.sharding import Mesh
from jax.sharding import PartitionSpec as P

FW = 11264
R = 512
AXES = ("y", "zr", "zl", "x", "c")
DP = ("y", "zr", "zl")
TENSOR = ("x", "c")
NEAR = ("y", "zl")
BF = jnp.bfloat16
F32 = jnp.float32


beta_one = 0.9
beta_two = 0.999
adam_eps = 1e-08
corr_one = 1.0 - 0.9**10
corr_two = 1.0 - 0.999**10
step_size = 0.002
decay_keep = 0.99


def exchange(x, axes):
    return lax.all_to_all(x, axes, split_axis=0, concat_axis=0, tiled=True)


def to_all(x, axes):
    n = math.prod(lax.axis_size(a) for a in axes)
    return exchange(jnp.broadcast_to(x, (n, *x.shape)), axes)


def flip_pairs():
    pairs = []
    for y in range(4):
        for z in range(16):
            for x in range(4):
                for c in range(2):
                    pairs.append((((y * 16 + z) * 4 + x) * 2 + c, ((x * 16 + z) * 4 + y) * 2 + c))
    return pairs


def adam_update(lowrank, square, first_moment, second_moment):
    bound_norm = math.sqrt(R * FW)
    factor = jnp.minimum(1.0, bound_norm / (jnp.sqrt(square) + 1e-06))
    clipped = lowrank * factor
    first = beta_one * first_moment + (1.0 - beta_one) * clipped
    second = beta_two * second_moment + (1.0 - beta_two) * clipped * clipped
    update = (first / corr_one / (jnp.sqrt(second / corr_two) + adam_eps)).astype(BF)
    return (first, second, update)


def on_device(inputs, out_grads, basis, weight, first_moment, second_moment):
    piece = basis.T.reshape(4, 2, 8, 128).transpose(1, 0, 2, 3).reshape(64, 128)
    flipped = lax.ppermute(piece, AXES, flip_pairs())
    far = to_all(flipped, ("zr",))
    halves = far.reshape(2, 1, 4, 64, 128)
    for_all = jnp.broadcast_to(halves.transpose(1, 0, 2, 3, 4), (8, 2, 4, 64, 128)).reshape(16, 4, 64, 128)
    arrived = exchange(for_all, ("y", "zl", "c"))
    slices = arrived.reshape(4, 2, 2, 4, 2, 32, 128)
    columns = slices.transpose(0, 4, 2, 5, 3, 1, 6).reshape(512, 1024)
    partial_value = lax.dot_general(
        inputs, columns, (((1,), (1,)), ((), ())), preferred_element_type=F32
    ).astype(BF)
    shares = exchange(partial_value.reshape(8, 72, 512), TENSOR)
    own_tokens = jnp.sum(shares.astype(F32), axis=0).astype(BF)
    wide = jnp.concatenate([piece[16 * k : 16 * k + 16] for k in range(4)], axis=1)
    both = to_all(jnp.concatenate([own_tokens, wide], axis=0), TENSOR)
    projected = both[:, :72].reshape(576, 512)
    back = both[:, 72:].reshape(8, 16, 4, 128).transpose(0, 2, 1, 3)
    back = back.reshape(4, 2, 2, 32, 128).transpose(0, 2, 1, 3, 4).reshape(512, 128)
    partial_low = lax.dot_general(
        projected, out_grads, (((0,), (0,)), ((), ())), preferred_element_type=F32
    ).astype(BF)
    near = exchange(partial_low.reshape(8, 64, 1408), NEAR)
    near_sum = jnp.sum(near.astype(F32), axis=0).astype(BF)
    own = exchange(near_sum.reshape(8, 8, 1408), ("zr",))
    own_rows = jnp.sum(own.astype(F32), axis=0)
    square = jnp.sum(own_rows * own_rows).reshape(1, 1)
    square = jnp.sum(to_all(square, ("y", "x", "c")), axis=0)
    square = jnp.sum(to_all(square, ("zr", "zl")), axis=0)
    first, second, update = adam_update(own_rows, square[0, 0], first_moment, second_moment)
    far_update = to_all(update, ("zr",)).reshape(64, 1408)
    all_update = to_all(far_update, NEAR).reshape(512, 1408)
    delta = lax.dot_general(back, all_update, (((0,), (0,)), ((), ())), preferred_element_type=F32)
    new_weight = (decay_keep * weight.astype(F32) - step_size * delta).astype(BF)
    return (new_weight, first, second)


def solution(mesh):
    torus = Mesh(mesh.devices.reshape(4, 8, 2, 4, 2), AXES)
    spec = P(DP, TENSOR)
    return jax.shard_map(
        on_device,
        mesh=torus,
        in_specs=(spec,) * 6,
        out_specs=(spec,) * 3,
        check_vma=False,
    )
```

```python
import math

import jax
import jax.numpy as jnp
from jax import lax
from jax.experimental import pallas as pl
from jax.experimental.pallas import tpu as pltpu
from jax.sharding import Mesh
from jax.sharding import PartitionSpec as P

FW = 11264
R = 512
AXES = ("y", "zr", "zl", "x", "c")
DP = ("y", "zr", "zl")
TENSOR = ("x", "c")
NEAR = ("y", "zl")
PLANE = ("y", "zl", "x", "c")
BF = jnp.bfloat16
F32 = jnp.float32


beta_one = 0.9
beta_two = 0.999
adam_eps = 1e-08
corr_one = 1.0 - 0.9**10
corr_two = 1.0 - 0.999**10
step_size = 0.002
decay_keep = 0.99


def exchange(x, axes):
    return lax.all_to_all(x, axes, split_axis=0, concat_axis=0, tiled=True)


def to_all(x, axes):
    n = math.prod(lax.axis_size(a) for a in axes)
    return exchange(jnp.broadcast_to(x, (n, *x.shape)), axes)


def shape(dims, dtype):
    return jax.ShapeDtypeStruct(dims, dtype)


def small(mib):
    return pltpu.CompilerParams(vmem_limit_bytes=mib * 2**20)


def project_kernel(inputs, blocks, out, columns):
    for y in range(4):
        for zl in range(2):
            for high in range(2):
                for mid in range(2):
                    row = 16 * (((y * 2 + zl) * 2 + high) * 2 + mid)
                    for f in range(8):
                        columns[row : row + 16, 128 * f : 128 * f + 128] = blocks[
                            zl * 2 + mid, f % 2, y, high, f // 2
                        ]
    out[...] = lax.dot_general(
        inputs[...], columns[...], (((1,), (1,)), ((), ())), preferred_element_type=F32
    ).astype(BF)


def project(inputs, blocks):
    return pl.pallas_call(
        project_kernel,
        out_shape=shape((576, 512), BF),
        scratch_shapes=[pltpu.VMEM((512, 1024), BF)],
        compiler_params=small(16),
        name="project",
    )(inputs, blocks)


def near_kernel(parts, out):
    out[...] = jnp.sum(parts[...].astype(F32), axis=0).astype(BF)


def near_sum(parts):
    return pl.pallas_call(
        near_kernel,
        out_shape=shape((64, 1408), BF),
        compiler_params=small(8),
        name="near_sum",
    )(parts)


def own_kernel(parts, rows, square):
    own = jnp.sum(parts[...].astype(F32), axis=0)
    rows[...] = own
    lanes = jnp.zeros((1, 128), F32)
    squares = own * own
    for k in range(11):
        lanes += jnp.sum(squares[:, 128 * k : 128 * k + 128], axis=0, keepdims=True)
    square[...] = jnp.broadcast_to(lanes[None], (64, 1, 128))


def own_sum(parts):
    return pl.pallas_call(
        own_kernel,
        out_shape=(shape((8, 1408), F32), shape((64, 1, 128), F32)),
        compiler_params=small(4),
        name="own_sum",
    )(parts)


def plane_kernel(parts, out):
    total = jnp.sum(parts[...], axis=0, keepdims=True)
    out[...] = jnp.broadcast_to(total, (8, 1, 128))


def plane_sum(parts):
    return pl.pallas_call(
        plane_kernel,
        out_shape=shape((8, 1, 128), F32),
        compiler_params=small(2),
        name="plane_sum",
    )(parts)


def adam_kernel(lowrank, square, first_moment, second_moment, new_first, new_second, update):
    bound_norm = math.sqrt(R * FW)
    total = jnp.sum(jnp.sum(square[...], axis=0), axis=1, keepdims=True)
    factor = jnp.minimum(1.0, bound_norm / (jnp.sqrt(total) + 1e-06))
    clipped = lowrank[...] * factor
    first = beta_one * first_moment[...] + (1.0 - beta_one) * clipped
    second = beta_two * second_moment[...] + (1.0 - beta_two) * clipped * clipped
    new_first[...] = first
    new_second[...] = second
    step = (first / corr_one / (jnp.sqrt(second / corr_two) + adam_eps)).astype(BF)
    for k in range(8):
        update[k] = step


def adam(lowrank, square, first_moment, second_moment):
    return pl.pallas_call(
        adam_kernel,
        out_shape=(shape((8, 1408), F32), shape((8, 1408), F32), shape((8, 8, 1408), BF)),
        compiler_params=small(4),
        name="adam",
    )(lowrank, square, first_moment, second_moment)


def apply_kernel(both, update, weight, out, back):
    for y in range(4):
        for high in range(2):
            for k in range(4):
                row = ((y * 2 + k // 2) * 2 + high) * 32 + (k % 2) * 16
                back[row : row + 16, :] = both[y * 2 + high, :16, 128 * k : 128 * k + 128]
    delta = lax.dot_general(
        back[...], update[...], (((0,), (0,)), ((), ())), preferred_element_type=F32
    )
    out[...] = (decay_keep * weight[...].astype(F32) - step_size * delta).astype(BF)


def apply_update(both, update, weight):
    return pl.pallas_call(
        apply_kernel,
        out_shape=shape((128, 1408), BF),
        scratch_shapes=[pltpu.VMEM((512, 128), BF)],
        compiler_params=small(12),
        name="apply_update",
    )(both, update, weight)


def on_device(inputs, out_grads, basis, weight, first_moment, second_moment):
    piece = basis.T.reshape(4, 2, 8, 128).transpose(1, 0, 2, 3).reshape(64, 128)
    quarters = jnp.broadcast_to(piece.reshape(4, 1, 16, 128), (4, 8, 16, 128))
    wide = jnp.concatenate([piece[16 * k : 16 * k + 16] for k in range(4)], axis=1)
    quarters, wide = lax.optimization_barrier((quarters, wide))
    far = exchange(quarters.reshape(32, 16, 128), ("y", "zr"))
    copies = jnp.broadcast_to(far.reshape(1, 8, 4, 16, 128), (8, 8, 4, 16, 128))
    slices = exchange(copies.reshape(64, 4, 16, 128), PLANE)
    partial_value = project(inputs, slices.reshape(4, 2, 4, 2, 4, 16, 128))
    shares = exchange(partial_value.reshape(8, 72, 512), TENSOR)
    own_tokens = jnp.sum(shares.astype(F32), axis=0).astype(BF)
    both = to_all(jnp.concatenate([wide, own_tokens], axis=0), TENSOR)
    projected = both[:, 16:].reshape(576, 512)
    partial_low = lax.dot_general(
        projected, out_grads, (((0,), (0,)), ((), ())), preferred_element_type=F32
    ).astype(BF)
    near = exchange(partial_low.reshape(8, 64, 1408), NEAR)
    own = exchange(near_sum(near).reshape(8, 8, 1408), ("zr",))
    own_rows, square = own_sum(own)
    square = plane_sum(exchange(square, PLANE))
    first, second, update = adam(own_rows, exchange(square, ("zr",)), first_moment, second_moment)
    far_update = exchange(update, ("zr",)).reshape(64, 1408)
    all_update = to_all(far_update, NEAR).reshape(512, 1408)
    new_weight = apply_update(both, all_update, weight)
    return (new_weight, first, second)


def solution(mesh):
    torus = Mesh(mesh.devices.reshape(4, 8, 2, 4, 2), AXES)
    spec = P(DP, TENSOR)
    return jax.shard_map(
        on_device,
        mesh=torus,
        in_specs=(spec,) * 6,
        out_specs=(spec,) * 3,
        check_vma=False,
    )
```

```python
import math

import jax
import jax.numpy as jnp
from jax import lax
from jax.experimental import pallas as pl
from jax.experimental.pallas import tpu as pltpu
from jax.sharding import Mesh
from jax.sharding import PartitionSpec as P


FW = 11264
R = 512
AXES = ("y", "zr", "zl", "x", "c")
DP = ("y", "zr", "zl")
TENSOR = ("x", "c")
NEAR = ("y", "zl")
PLANE = ("y", "zl", "x", "c")
BF = jnp.bfloat16
F32 = jnp.float32


beta_one = 0.9
beta_two = 0.999
adam_eps = 1e-08
corr_one = 1.0 - 0.9**10
corr_two = 1.0 - 0.999**10
step_size = 0.002
decay_keep = 0.99


def exchange(x, axes):
    return lax.all_to_all(x, axes, split_axis=0, concat_axis=0, tiled=True)


def to_all(x, axes):
    n = math.prod(lax.axis_size(a) for a in axes)
    return exchange(jnp.broadcast_to(x, (n, *x.shape)), axes)


def shape(dims, dtype):
    return jax.ShapeDtypeStruct(dims, dtype)


def small(mib):
    return pltpu.CompilerParams(vmem_limit_bytes=mib * 2**20)


def project_kernel(inputs, blocks, wide, out, columns):
    for zl in range(2):
        for y in range(4):
            for high in range(2):
                for mid in range(2):
                    row = 16 * (((zl * 4 + y) * 2 + high) * 2 + mid)
                    for f in range(8):
                        columns[row : row + 16, 128 * f : 128 * f + 128] = blocks[
                            zl * 2 + mid, f % 2, y, high, f // 2
                        ]
    partial_value = lax.dot_general(
        inputs[...], columns[...], (((1,), (1,)), ((), ())), preferred_element_type=F32
    )
    for t in range(8):
        out[t, :16] = wide[...]
        out[t, 16:] = partial_value[72 * t : 72 * t + 72].astype(BF)


def project(inputs, blocks, wide):
    return pl.pallas_call(
        project_kernel,
        out_shape=shape((8, 88, 512), BF),
        scratch_shapes=[pltpu.VMEM((512, 1024), BF)],
        compiler_params=small(16),
        name="project",
    )(inputs, blocks, wide)


def lowrank_kernel(parity, tokens, own_grads, pair_grads, out):
    contract = (((0,), (0,)), ((), ()))
    own = lax.dot_general(tokens[parity[0]], own_grads[...], contract, preferred_element_type=F32)
    pair = lax.dot_general(tokens[1 - parity[0]], pair_grads[...], contract, preferred_element_type=F32)
    out[...] = (own + pair).astype(BF)


def pair_lowrank(parity, tokens, own_grads, pair_grads):
    whole = pl.BlockSpec(memory_space=pltpu.VMEM)
    return pl.pallas_call(
        lowrank_kernel,
        in_specs=[pl.BlockSpec(memory_space=pltpu.SMEM), whole, whole, whole],
        out_shape=shape((256, 1408), BF),
        compiler_params=small(16),
        name="pair_lowrank",
    )(parity, tokens, own_grads, pair_grads)


def near_kernel(parts, out):
    out[...] = jnp.sum(parts[...].astype(F32), axis=0).astype(BF)


def near_sum(parts):
    return pl.pallas_call(
        near_kernel,
        out_shape=shape((64, 1408), BF),
        compiler_params=small(8),
        name="near_sum",
    )(parts)


def own_kernel(parts, rows, square):
    own = jnp.sum(parts[...].astype(F32), axis=0)
    rows[...] = own
    lanes = jnp.zeros((1, 128), F32)
    squares = own * own
    for k in range(11):
        lanes += jnp.sum(squares[:, 128 * k : 128 * k + 128], axis=0, keepdims=True)
    square[...] = jnp.broadcast_to(lanes[None], (64, 1, 128))


def own_sum(parts):
    return pl.pallas_call(
        own_kernel,
        out_shape=(shape((8, 1408), F32), shape((64, 1, 128), F32)),
        compiler_params=small(4),
        name="own_sum",
    )(parts)


def plane_kernel(parts, out):
    total = jnp.sum(parts[...], axis=0, keepdims=True)
    out[...] = jnp.broadcast_to(total, (8, 1, 128))


def plane_sum(parts):
    return pl.pallas_call(
        plane_kernel,
        out_shape=shape((8, 1, 128), F32),
        compiler_params=small(2),
        name="plane_sum",
    )(parts)


def adam_kernel(lowrank, square, first_moment, second_moment, new_first, new_second, update):
    bound_norm = math.sqrt(R * FW)
    total = jnp.sum(jnp.sum(square[...], axis=0), axis=1, keepdims=True)
    factor = jnp.minimum(1.0, bound_norm / (jnp.sqrt(total) + 1e-06))
    clipped = lowrank[...] * factor
    first = beta_one * first_moment[...] + (1.0 - beta_one) * clipped
    second = beta_two * second_moment[...] + (1.0 - beta_two) * clipped * clipped
    new_first[...] = first
    new_second[...] = second
    step = (first / corr_one / (jnp.sqrt(second / corr_two) + adam_eps)).astype(BF)
    for k in range(8):
        update[k] = step


def adam(lowrank, square, first_moment, second_moment):
    return pl.pallas_call(
        adam_kernel,
        out_shape=(shape((8, 1408), F32), shape((8, 1408), F32), shape((8, 8, 1408), BF)),
        compiler_params=small(4),
        name="adam",
    )(lowrank, square, first_moment, second_moment)


def apply_kernel(both, update, weight, out, back):
    for y in range(4):
        for high in range(2):
            for k in range(4):
                row = ((y * 2 + k // 2) * 2 + high) * 32 + (k % 2) * 16
                back[row : row + 16, :] = both[y * 2 + high, :16, 128 * k : 128 * k + 128]
    delta = lax.dot_general(
        back[...], update[...], (((0,), (0,)), ((), ())), preferred_element_type=F32
    )
    out[...] = (decay_keep * weight[...].astype(F32) - step_size * delta).astype(BF)


def apply_update(both, update, weight):
    return pl.pallas_call(
        apply_kernel,
        out_shape=shape((128, 1408), BF),
        scratch_shapes=[pltpu.VMEM((512, 128), BF)],
        compiler_params=small(12),
        name="apply_update",
    )(both, update, weight)


def body(inputs, out_grads, basis, weight, first_moment, second_moment):
    pair_grads = lax.ppermute(out_grads, "zl", [(0, 1), (1, 0)])
    parity = lax.axis_index("zl").reshape(1)
    piece = basis.T.reshape(4, 2, 8, 128).transpose(1, 0, 2, 3).reshape(64, 128)
    quarters = jnp.broadcast_to(piece.reshape(4, 1, 16, 128), (4, 8, 16, 128))
    wide = jnp.concatenate([piece[16 * k : 16 * k + 16] for k in range(4)], axis=1)
    quarters, wide, parity = lax.optimization_barrier((quarters, wide, parity))
    far = exchange(quarters.reshape(32, 16, 128), ("y", "zr"))
    copies = jnp.broadcast_to(far.reshape(1, 8, 4, 16, 128), (8, 8, 4, 16, 128))
    slices = exchange(copies.reshape(64, 4, 16, 128), PLANE)
    partial_value = project(inputs, slices.reshape(4, 2, 4, 2, 4, 16, 128), wide)
    partial_value, pair_grads = lax.optimization_barrier((partial_value, pair_grads))
    shares = exchange(partial_value, TENSOR)
    own_tokens = jnp.sum(shares[:, 16:].astype(F32), axis=0).astype(BF)
    halves = [jnp.broadcast_to(own_tokens[:, 256 * k : 256 * k + 256], (8, 72, 256)) for k in range(2)]
    tokens = exchange(jnp.concatenate(halves), ("zl", "x", "c")).reshape(2, 576, 256)
    partial_low = pair_lowrank(parity, tokens, out_grads, pair_grads)
    near = exchange(partial_low.reshape(4, 64, 1408), ("y",))
    own = exchange(near_sum(near).reshape(8, 8, 1408), ("zr",))
    own_rows, square = own_sum(own)
    square = plane_sum(exchange(square, PLANE))
    first, second, update = adam(own_rows, exchange(square, ("zr",)), first_moment, second_moment)
    far_update = exchange(update, ("zr",)).reshape(64, 1408)
    all_update = to_all(far_update, NEAR).reshape(512, 1408)
    new_weight = apply_update(shares, all_update, weight)
    return (new_weight, first, second)


def solution(mesh):
    torus = Mesh(mesh.devices.reshape(4, 8, 2, 4, 2), AXES)
    spec = P(DP, TENSOR)
    return jax.shard_map(
        body,
        mesh=torus,
        in_specs=(spec,) * 6,
        out_specs=(spec,) * 3,
        check_vma=False,
    )
```

```python
import math

import jax
import jax.numpy as jnp
from jax import lax
from jax.experimental import pallas as pl
from jax.experimental.pallas import tpu as pltpu
from jax.sharding import Mesh
from jax.sharding import PartitionSpec as P


FW = 11264
R = 512
AXES = ("y", "zr", "zl", "x", "c")
DP = ("y", "zr", "zl")
TENSOR = ("x", "c")
NEAR = ("y", "zl")
PLANE = ("y", "zl", "x", "c")
BF = jnp.bfloat16
F32 = jnp.float32


beta_one = 0.9
beta_two = 0.999
adam_eps = 1e-08
corr_one = 1.0 - 0.9**10
corr_two = 1.0 - 0.999**10
step_size = 0.002
decay_keep = 0.99


def exchange(x, axes):
    return lax.all_to_all(x, axes, split_axis=0, concat_axis=0, tiled=True)


def across(bit):
    return [(i, i ^ bit) for i in range(8)]


def shape(dims, dtype):
    return jax.ShapeDtypeStruct(dims, dtype)


def small(mib):
    return pltpu.CompilerParams(vmem_limit_bytes=mib * 2**20)


def project_kernel(inputs, blocks, out, columns):
    for y in range(4):
        for zl in range(2):
            for high in range(2):
                for mid in range(2):
                    row = 16 * (((y * 2 + zl) * 2 + high) * 2 + mid)
                    for f in range(8):
                        columns[row : row + 16, 128 * f : 128 * f + 128] = blocks[
                            zl * 2 + mid, f % 2, y, high, f // 2
                        ]
    out[...] = lax.dot_general(
        inputs[...], columns[...], (((1,), (1,)), ((), ())), preferred_element_type=F32
    ).astype(BF)


def project(inputs, blocks):
    return pl.pallas_call(
        project_kernel,
        out_shape=shape((576, 512), BF),
        scratch_shapes=[pltpu.VMEM((512, 1024), BF)],
        compiler_params=small(16),
        name="project",
    )(inputs, blocks)


def near_kernel(parts, out):
    out[...] = jnp.sum(parts[...].astype(F32), axis=0).astype(BF)


def near_sum(parts):
    return pl.pallas_call(
        near_kernel,
        out_shape=shape((64, 1408), BF),
        compiler_params=small(8),
        name="near_sum",
    )(parts)


def own_kernel(parts, rows, shared):
    own = jnp.sum(parts[...].astype(F32), axis=0)
    rows[...] = own
    squares = own * own
    lanes = jnp.zeros((1, 128), F32)
    for k in range(11):
        lanes += jnp.sum(squares[:, 128 * k : 128 * k + 128], axis=0, keepdims=True)
    high = lanes.astype(BF).astype(F32)
    at = lax.broadcasted_iota(jnp.int32, (8, 128), 0)
    split = jnp.where(at == 0, high, jnp.where(at == 1, lanes - high, 0.0)).astype(BF)
    rounded = own.astype(BF)
    for k in range(8):
        shared[k, :, :1408] = rounded
        shared[k, :, 1408:] = split


def own_sum(parts):
    return pl.pallas_call(
        own_kernel,
        out_shape=(shape((8, 1408), F32), shape((8, 8, 1536), BF)),
        compiler_params=small(4),
        name="own_sum",
    )(parts)


def far_kernel(shared, out):
    lanes = jnp.sum(jnp.sum(shared[:, :, 1408:].astype(F32), axis=0), axis=0, keepdims=True)
    out[...] = jnp.broadcast_to(lanes[None], (64, 1, 128))


def far_square(shared):
    return pl.pallas_call(
        far_kernel,
        out_shape=shape((64, 1, 128), F32),
        compiler_params=small(2),
        name="far_square",
    )(shared)


def adam_kernel(
    index, lowrank, first_moment, second_moment, square, shared, even, odd, new_first, new_second, update
):
    bound_norm = math.sqrt(R * FW)
    total = jnp.sum(jnp.sum(square[...], axis=0), axis=1, keepdims=True)
    factor = jnp.minimum(1.0, bound_norm / (jnp.sqrt(total) + 1e-06))

    def averages(rows, m, v):
        clipped = rows * factor
        first = beta_one * m + (1.0 - beta_one) * clipped
        return first, beta_two * v + (1.0 - beta_two) * clipped * clipped

    new_first[...], new_second[...] = averages(lowrank[...], first_moment[...], second_moment[...])
    for k in range(8):
        moments = (even, odd)[k % 2]
        at = (k // 2) % 2 * 2 + k // 4
        z = index[0] ^ k
        first, second = averages(
            shared[z, :, :1408].astype(F32), moments[at, 0].astype(F32), moments[at, 1].astype(F32)
        )
        step = (first / corr_one / (jnp.sqrt(second / corr_two) + adam_eps)).astype(BF)
        for copy in range(8):
            update[copy, z] = step


def adam(*args):
    whole = pl.BlockSpec(memory_space=pltpu.VMEM)
    return pl.pallas_call(
        adam_kernel,
        in_specs=[pl.BlockSpec(memory_space=pltpu.SMEM)] + [whole] * 7,
        out_shape=(shape((8, 1408), F32), shape((8, 1408), F32), shape((8, 8, 8, 1408), BF)),
        compiler_params=small(8),
        name="adam",
    )(*args)


def apply_kernel(both, update, decayed, out, back):
    for y in range(4):
        for high in range(2):
            for k in range(4):
                row = ((y * 2 + k // 2) * 2 + high) * 32 + (k % 2) * 16
                back[row : row + 16, :] = both[y * 2 + high, :16, 128 * k : 128 * k + 128]
    delta = lax.dot_general(
        back[...], update[...], (((0,), (0,)), ((), ())), preferred_element_type=F32
    )
    out[...] = (decayed[...] - step_size * delta).astype(BF)


def apply_update(both, update, decayed):
    return pl.pallas_call(
        apply_kernel,
        out_shape=shape((128, 1408), BF),
        scratch_shapes=[pltpu.VMEM((512, 128), BF)],
        compiler_params=small(12),
        name="apply_update",
    )(both, update, decayed)


def body(inputs, out_grads, basis, weight, first_moment, second_moment):
    piece = basis.T.reshape(4, 2, 8, 128).transpose(1, 0, 2, 3).reshape(64, 128)
    quarters = jnp.broadcast_to(piece.reshape(4, 1, 16, 128), (4, 8, 16, 128))
    index = lax.axis_index("zr").reshape(1)
    quarters, index = lax.optimization_barrier((quarters, index))
    far = exchange(quarters.reshape(32, 16, 128), ("y", "zr"))
    copies = jnp.broadcast_to(far.reshape(1, 8, 4, 16, 128), (8, 8, 4, 16, 128))
    slices = exchange(copies.reshape(64, 4, 16, 128), PLANE)
    partial_value = project(inputs, slices.reshape(4, 2, 4, 2, 4, 16, 128))
    shares = exchange(partial_value.reshape(8, 72, 512), TENSOR)
    wide = jnp.concatenate([piece[16 * k : 16 * k + 16] for k in range(4)], axis=1)
    moments = jnp.stack([first_moment, second_moment]).astype(BF)
    other = lax.ppermute(moments, "zr", across(4))
    moments = jnp.stack([moments, other])
    second = lax.ppermute(moments, "zr", across(2))
    own_tokens = jnp.sum(shares.astype(F32), axis=0).astype(BF)
    own_tokens = jnp.broadcast_to(jnp.concatenate([wide, own_tokens], axis=0), (8, 88, 512))
    both = exchange(own_tokens, TENSOR)
    decayed = decay_keep * weight.astype(F32)
    projected = both[:, 16:].reshape(576, 512)
    partial_low = lax.dot_general(
        projected, out_grads, (((0,), (0,)), ((), ())), preferred_element_type=F32
    ).astype(BF)
    near = exchange(partial_low.reshape(8, 64, 1408), NEAR)
    own = exchange(near_sum(near).reshape(8, 8, 1408), ("zr",))
    own_rows, shared = own_sum(own)
    shared = exchange(shared, ("zr",))
    square = far_square(shared)
    square = exchange(square, PLANE)
    even = jnp.concatenate([moments, second])
    odd = lax.ppermute(even, "zr", across(1))
    first, second, update = adam(index, own_rows, first_moment, second_moment, square, shared, even, odd)
    all_update = exchange(update.reshape(8, 64, 1408), NEAR).reshape(512, 1408)
    new_weight = apply_update(both, all_update, decayed)
    return (new_weight, first, second)


def solution(mesh):
    torus = Mesh(mesh.devices.reshape(4, 8, 2, 4, 2), AXES)
    spec = P(DP, TENSOR)
    return jax.shard_map(
        body,
        mesh=torus,
        in_specs=(spec,) * 6,
        out_specs=(spec,) * 3,
        check_vma=False,
    )
```

```python
import math

import jax
import jax.numpy as jnp
from jax import lax
from jax.experimental import pallas as pl
from jax.experimental.pallas import tpu as pltpu
from jax.sharding import Mesh
from jax.sharding import PartitionSpec as P

FW = 11264
R = 512
AXES = ("y", "zr", "zl", "x", "c")
DP = ("y", "zr", "zl")
TENSOR = ("x", "c")
SHARES = ("c", "x")
NEAR = ("zl", "y")
PLANE = ("y", "zl", "x", "c")
BF = jnp.bfloat16
F32 = jnp.float32


beta_one = 0.9
beta_two = 0.999
adam_eps = 1e-08
corr_one = 1.0 - 0.9**10
corr_two = 1.0 - 0.999**10
step_size = 0.002
decay_keep = 0.99


def exchange(x, axes):
    return lax.all_to_all(x, axes, split_axis=0, concat_axis=0, tiled=True)


def to_all(x, axes):
    n = math.prod(lax.axis_size(a) for a in axes)
    return exchange(jnp.broadcast_to(x, (n, *x.shape)), axes)


def shape(dims, dtype):
    return jax.ShapeDtypeStruct(dims, dtype)


def small(mib):
    return pltpu.CompilerParams(vmem_limit_bytes=mib * 2**20)


def project_kernel(inputs, blocks, out, columns):
    for zl in range(2):
        for y in range(4):
            for high in range(2):
                for mid in range(2):
                    row = 16 * (((zl * 4 + y) * 2 + high) * 2 + mid)
                    for f in range(8):
                        columns[row : row + 16, 128 * f : 128 * f + 128] = blocks[
                            zl * 2 + mid, f % 2, y, high, f // 2
                        ]
    out[...] = lax.dot_general(
        inputs[...], columns[...], (((1,), (1,)), ((), ())), preferred_element_type=F32
    ).astype(BF)


def project(inputs, blocks):
    return pl.pallas_call(
        project_kernel,
        out_shape=shape((576, 512), BF),
        scratch_shapes=[pltpu.VMEM((512, 1024), BF)],
        compiler_params=small(16),
        name="project",
    )(inputs, blocks)


def near_kernel(parts, out):
    out[...] = jnp.sum(parts[...].astype(F32), axis=0).astype(BF)


def near_sum(parts):
    return pl.pallas_call(
        near_kernel,
        out_shape=shape((64, 1408), BF),
        compiler_params=small(8),
        name="near_sum",
    )(parts)


def own_kernel(parts, rows, square):
    own = jnp.sum(parts[...].astype(F32), axis=0)
    rows[...] = own
    lanes = jnp.zeros((1, 128), F32)
    squares = own * own
    for k in range(11):
        lanes += jnp.sum(squares[:, 128 * k : 128 * k + 128], axis=0, keepdims=True)
    square[...] = jnp.broadcast_to(lanes[None], (64, 1, 128))


def own_sum(parts):
    return pl.pallas_call(
        own_kernel,
        out_shape=(shape((8, 1408), F32), shape((64, 1, 128), F32)),
        compiler_params=small(4),
        name="own_sum",
    )(parts)


def plane_kernel(parts, out):
    total = jnp.sum(parts[...], axis=0, keepdims=True)
    out[...] = jnp.broadcast_to(total, (8, 1, 128))


def plane_sum(parts):
    return pl.pallas_call(
        plane_kernel,
        out_shape=shape((8, 1, 128), F32),
        compiler_params=small(2),
        name="plane_sum",
    )(parts)


def adam_kernel(lowrank, square, first_moment, second_moment, new_first, new_second, update):
    bound_norm = math.sqrt(R * FW)
    total = jnp.sum(jnp.sum(square[...], axis=0), axis=1, keepdims=True)
    factor = jnp.minimum(1.0, bound_norm / (jnp.sqrt(total) + 1e-06))
    clipped = lowrank[...] * factor
    first = beta_one * first_moment[...] + (1.0 - beta_one) * clipped
    second = beta_two * second_moment[...] + (1.0 - beta_two) * clipped * clipped
    new_first[...] = first
    new_second[...] = second
    step = (first / corr_one / (jnp.sqrt(second / corr_two) + adam_eps)).astype(BF)
    for k in range(8):
        update[k] = step


def adam(lowrank, square, first_moment, second_moment):
    return pl.pallas_call(
        adam_kernel,
        out_shape=(shape((8, 1408), F32), shape((8, 1408), F32), shape((8, 8, 1408), BF)),
        compiler_params=small(4),
        name="adam",
    )(lowrank, square, first_moment, second_moment)


def apply_kernel(both, update, weight, out, back):
    for y in range(4):
        for high in range(2):
            for k in range(4):
                row = ((k // 2 * 4 + y) * 2 + high) * 32 + (k % 2) * 16
                back[row : row + 16, :] = both[high * 4 + y, :16, 128 * k : 128 * k + 128]
    delta = lax.dot_general(
        back[...], update[...], (((0,), (0,)), ((), ())), preferred_element_type=F32
    )
    out[...] = (decay_keep * weight[...].astype(F32) - step_size * delta).astype(BF)


def apply_update(both, update, weight):
    return pl.pallas_call(
        apply_kernel,
        out_shape=shape((128, 1408), BF),
        scratch_shapes=[pltpu.VMEM((512, 128), BF)],
        compiler_params=small(12),
        name="apply_update",
    )(both, update, weight)


def on_device(inputs, out_grads, basis, weight, first_moment, second_moment):
    piece = basis.T.reshape(4, 2, 8, 128).transpose(1, 0, 2, 3).reshape(64, 128)
    quarters = jnp.broadcast_to(piece.reshape(4, 1, 16, 128), (4, 8, 16, 128))
    wide = jnp.concatenate([piece[16 * k : 16 * k + 16] for k in range(4)], axis=1)
    quarters, wide = lax.optimization_barrier((quarters, wide))
    far = exchange(quarters.reshape(32, 16, 128), ("y", "zr"))
    copies = jnp.broadcast_to(far.reshape(1, 8, 4, 16, 128), (8, 8, 4, 16, 128))
    slices = exchange(copies.reshape(64, 4, 16, 128), PLANE)
    partial_value = project(inputs, slices.reshape(4, 2, 4, 2, 4, 16, 128))
    shares = exchange(partial_value.reshape(8, 72, 512), SHARES)
    own_tokens = jnp.sum(shares.astype(F32), axis=0).astype(BF)
    both = to_all(jnp.concatenate([wide, own_tokens], axis=0), SHARES)
    projected = both[:, 16:].reshape(576, 512)
    partial_low = lax.dot_general(
        projected, out_grads, (((0,), (0,)), ((), ())), preferred_element_type=F32
    ).astype(BF)
    near = exchange(partial_low.reshape(8, 64, 1408), NEAR)
    own = exchange(near_sum(near).reshape(8, 8, 1408), ("zr",))
    own_rows, square = own_sum(own)
    square = plane_sum(exchange(square, PLANE))
    first, second, update = adam(own_rows, exchange(square, ("zr",)), first_moment, second_moment)
    far_update = exchange(update, ("zr",)).reshape(64, 1408)
    all_update = to_all(far_update, NEAR).reshape(512, 1408)
    new_weight = apply_update(both, all_update, weight)
    return (new_weight, first, second)


def solution(mesh):
    torus = Mesh(mesh.devices.reshape(4, 8, 2, 4, 2), AXES)
    spec = P(DP, TENSOR)
    return jax.shard_map(
        on_device,
        mesh=torus,
        in_specs=(spec,) * 6,
        out_specs=(spec,) * 3,
        check_vma=False,
    )
```

```python
import math

import jax
import jax.numpy as jnp
from jax import lax
from jax.experimental import pallas as pl
from jax.experimental.pallas import tpu as pltpu
from jax.sharding import Mesh
from jax.sharding import PartitionSpec as P

FW = 11264
R = 512
AXES = ("y", "zr", "zl", "x", "c")
DP = ("y", "zr", "zl")
TENSOR = ("x", "c")
SHARES = ("c", "x")
NEAR = ("zl", "y")
PLANE = ("y", "zl", "x", "c")
BF = jnp.bfloat16
F32 = jnp.float32


beta_one = 0.9
beta_two = 0.999
adam_eps = 1e-08
corr_one = 1.0 - 0.9**10
corr_two = 1.0 - 0.999**10
step_size = 0.002
decay_keep = 0.99


def exchange(x, axes):
    return lax.all_to_all(x, axes, split_axis=0, concat_axis=0, tiled=True)


def to_all(x, axes):
    n = math.prod(lax.axis_size(a) for a in axes)
    return exchange(jnp.broadcast_to(x, (n, *x.shape)), axes)


def shape(dims, dtype):
    return jax.ShapeDtypeStruct(dims, dtype)


def small(mib):
    return pltpu.CompilerParams(vmem_limit_bytes=mib * 2**20)


def project_kernel(inputs, blocks, out, columns):
    for zl in range(2):
        for y in range(4):
            for high in range(2):
                for mid in range(2):
                    row = 16 * (((zl * 4 + y) * 2 + high) * 2 + mid)
                    for f in range(8):
                        columns[row : row + 16, 128 * f : 128 * f + 128] = blocks[
                            zl * 2 + mid, f % 2, y, high, f // 2
                        ]
    out[...] = lax.dot_general(
        inputs[...], columns[...], (((1,), (1,)), ((), ())), preferred_element_type=F32
    ).astype(BF)


def project(inputs, blocks):
    return pl.pallas_call(
        project_kernel,
        out_shape=shape((576, 512), BF),
        scratch_shapes=[pltpu.VMEM((512, 1024), BF)],
        compiler_params=small(16),
        name="project",
    )(inputs, blocks)


def near_kernel(parts, out):
    out[...] = jnp.sum(parts[...].astype(F32), axis=0).astype(BF)


def near_sum(parts):
    return pl.pallas_call(
        near_kernel,
        out_shape=shape((64, 1408), BF),
        compiler_params=small(8),
        name="near_sum",
    )(parts)


def own_kernel(parts, rows, square):
    own = jnp.sum(parts[...].astype(F32), axis=0)
    rows[...] = own
    lanes = jnp.zeros((1, 128), F32)
    squares = own * own
    for k in range(11):
        lanes += jnp.sum(squares[:, 128 * k : 128 * k + 128], axis=0, keepdims=True)
    square[...] = jnp.broadcast_to(lanes[None], (32, 1, 128))


def own_sum(parts):
    return pl.pallas_call(
        own_kernel,
        out_shape=(shape((8, 1408), F32), shape((32, 1, 128), F32)),
        compiler_params=small(4),
        name="own_sum",
    )(parts)


def plane_kernel(parts, out):
    total = jnp.sum(parts[...], axis=0, keepdims=True)
    out[...] = jnp.broadcast_to(total, (16, 1, 128))


def plane_sum(parts):
    return pl.pallas_call(
        plane_kernel,
        out_shape=shape((16, 1, 128), F32),
        compiler_params=small(2),
        name="plane_sum",
    )(parts)


def averages(lowrank, square, first_moment, second_moment):
    bound_norm = math.sqrt(R * FW)
    total = jnp.sum(jnp.sum(square[...], axis=0), axis=1, keepdims=True)
    factor = jnp.minimum(1.0, bound_norm / (jnp.sqrt(total) + 1e-06))
    clipped = lowrank[...] * factor
    first = beta_one * first_moment[...] + (1.0 - beta_one) * clipped
    second = beta_two * second_moment[...] + (1.0 - beta_two) * clipped * clipped
    return first, second


def adam_kernel(lowrank, square, first_moment, second_moment, update):
    first, second = averages(lowrank, square, first_moment, second_moment)
    step = (first / corr_one / (jnp.sqrt(second / corr_two) + adam_eps)).astype(BF)
    for k in range(8):
        update[k] = step


def adam(*args):
    return pl.pallas_call(
        adam_kernel,
        out_shape=shape((8, 8, 1408), BF),
        compiler_params=small(4),
        name="adam",
    )(*args)


def apply_kernel(
    both, update, weight, lowrank, square, first_moment, second_moment, out, new_first, new_second, back
):
    for y in range(4):
        for high in range(2):
            for k in range(4):
                row = ((k // 2 * 4 + y) * 2 + high) * 32 + (k % 2) * 16
                back[row : row + 16, :] = both[high * 4 + y, :16, 128 * k : 128 * k + 128]
    delta = lax.dot_general(
        back[...], update[...], (((0,), (0,)), ((), ())), preferred_element_type=F32
    )
    out[...] = (decay_keep * weight[...].astype(F32) - step_size * delta).astype(BF)
    new_first[...], new_second[...] = averages(lowrank, square, first_moment, second_moment)


def apply_update(*args):
    return pl.pallas_call(
        apply_kernel,
        out_shape=(shape((128, 1408), BF), shape((8, 1408), F32), shape((8, 1408), F32)),
        scratch_shapes=[pltpu.VMEM((512, 128), BF)],
        compiler_params=small(12),
        name="apply_update",
    )(*args)


def on_device(inputs, out_grads, basis, weight, first_moment, second_moment):
    piece = basis.T.reshape(4, 2, 8, 128).transpose(1, 0, 2, 3).reshape(64, 128)
    quarters = jnp.broadcast_to(piece.reshape(4, 1, 16, 128), (4, 8, 16, 128))
    wide = jnp.concatenate([piece[16 * k : 16 * k + 16] for k in range(4)], axis=1)
    quarters, wide = lax.optimization_barrier((quarters, wide))
    far = exchange(quarters.reshape(32, 16, 128), ("y", "zr"))
    copies = jnp.broadcast_to(far.reshape(1, 8, 4, 16, 128), (8, 8, 4, 16, 128))
    slices = exchange(copies.reshape(64, 4, 16, 128), PLANE)
    partial_value = project(inputs, slices.reshape(4, 2, 4, 2, 4, 16, 128))
    shares = exchange(partial_value.reshape(8, 72, 512), SHARES)
    own_tokens = jnp.sum(shares.astype(F32), axis=0).astype(BF)
    both = to_all(jnp.concatenate([wide, own_tokens], axis=0), SHARES)
    projected = both[:, 16:].reshape(576, 512)
    partial_low = lax.dot_general(
        projected, out_grads, (((0,), (0,)), ((), ())), preferred_element_type=F32
    ).astype(BF)
    near = exchange(partial_low.reshape(8, 64, 1408), NEAR)
    own = exchange(near_sum(near).reshape(8, 8, 1408), ("zr",))
    own_rows, square = own_sum(own)
    square = plane_sum(exchange(square, ("y", "x", "c")))
    square = exchange(square, ("zr", "zl"))
    update = adam(own_rows, square, first_moment, second_moment)
    far_update = exchange(update, ("zr",)).reshape(64, 1408)
    all_update = to_all(far_update, NEAR).reshape(512, 1408)
    return apply_update(both, all_update, weight, own_rows, square, first_moment, second_moment)


def solution(mesh):
    torus = Mesh(mesh.devices.reshape(4, 8, 2, 4, 2), AXES)
    spec = P(DP, TENSOR)
    return jax.shard_map(
        on_device,
        mesh=torus,
        in_specs=(spec,) * 6,
        out_specs=(spec,) * 3,
        check_vma=False,
    )
```
